128 devices in a mesh: lat: 8 (over x, core), lon: 4 (over y), lev: 4 (over z).
Axes of the slice: x: 4, y: 4, z: 4, core: 2. Of those that a mesh axis runs over, the one named last changes fastest.
Arguments:
- initial_state: float32 [32, 384, 128, 128], P('lat', 'lon', 'lev'), may hold values from 0.5 to 2
- scaled_wind_north: float32 [32, 384, 128, 128], P('lat', 'lon', 'lev'), may hold values from -0.3 to 0.3
- scaled_wind_east: float32 [32, 384, 128, 128], P('lat', 'lon', 'lev'), may hold values from -0.3 to 0.3
- scaled_wind_upward: float32 [32, 384, 128, 128], P('lat', 'lon', 'lev'), may hold values from -0.3 to 0.3
Outputs:
- normalised_state: float32 [32, 384, 128, 128], P('lat', 'lon', 'lev')
- temperature_end: float32 [32, 384, 128, 128], P('lat', 'lon', 'lev')
The draws below stay inside these ranges and needn't reach their ends.
All inputs are finite; a program needn't handle non-finite values.
Results may differ from the reference program's by a relative error of at most 0.00002.
Values sent between devices are 32-bit elements; how exact they have to be, the bound alone decides.
A program may use at most 128 MiB of HBM per device.

```python
import jax
import jax.numpy as jnp
from jax import lax

CELLS_NORTHWARD = 32
CELLS_EASTWARD = 384
CELLS_UPWARD = 128
MEMBER_TOTAL = 128
STEPS = 4


def block_scale(rng, extent, pieces, low, high):
    def one(position, blocks):
        steps = jax.random.uniform(jax.random.fold_in(jax.random.fold_in(rng, 6), position), (blocks,), jnp.float32, low / len(pieces), high / len(pieces))
        return jnp.repeat(jnp.exp(steps), extent[position] // blocks).reshape((-1,) + (1,) * (len(extent) - position - 1))

    gain = one(*pieces[0])
    for cut in pieces[1:]:
        gain = gain * one(*cut)
    return gain


def setup_inputs(seed: int = 0) -> dict:
    key_of = jax.random.split(jax.random.key(seed), 5)
    return {
        "initial_state": jnp.clip(0.5 + 1.5 * jax.random.uniform(key_of[0], (CELLS_NORTHWARD, CELLS_EASTWARD, CELLS_UPWARD, MEMBER_TOTAL), jnp.float32) ** block_scale(key_of[0], (CELLS_NORTHWARD, CELLS_EASTWARD, CELLS_UPWARD, MEMBER_TOTAL), ((0, 8), (1, 4), (2, 4)), -0.2, 0.2), 0.5, 2.0),
        "scaled_wind_north": jnp.clip(jax.random.uniform(key_of[1], (CELLS_NORTHWARD, CELLS_EASTWARD, CELLS_UPWARD, MEMBER_TOTAL), jnp.float32, -0.3, 0.3) * block_scale(key_of[1], (CELLS_NORTHWARD, CELLS_EASTWARD, CELLS_UPWARD, MEMBER_TOTAL), ((0, 8), (1, 4), (2, 4)), -0.4, 0.0), -0.3, 0.3),
        "scaled_wind_east": jnp.clip(jax.random.uniform(key_of[2], (CELLS_NORTHWARD, CELLS_EASTWARD, CELLS_UPWARD, MEMBER_TOTAL), jnp.float32, -0.3, 0.3) * block_scale(key_of[2], (CELLS_NORTHWARD, CELLS_EASTWARD, CELLS_UPWARD, MEMBER_TOTAL), ((0, 8), (1, 4), (2, 4)), -0.4, 0.0), -0.3, 0.3),
        "scaled_wind_upward": jnp.clip(jax.random.uniform(key_of[3], (CELLS_NORTHWARD, CELLS_EASTWARD, CELLS_UPWARD, MEMBER_TOTAL), jnp.float32, -0.3, 0.3) * block_scale(key_of[3], (CELLS_NORTHWARD, CELLS_EASTWARD, CELLS_UPWARD, MEMBER_TOTAL), ((0, 8), (1, 4), (2, 4)), -0.4, 0.0), -0.3, 0.3),
    }


def strip_edges(values, dims):
    for dim in dims:
        values = lax.slice_in_dim(values, 1, values.shape[dim] - 1, axis=dim)
    return values

def neighbour(values, dim, start, dims):
    others = [other for other in dims if other != dim]
    values = strip_edges(values, others)
    return lax.slice_in_dim(values, start, start + values.shape[dim] - 2, axis=dim)

def march_one_step(padded_state, scaled_wind_north, scaled_wind_east, scaled_wind_upward):
    middle = strip_edges(padded_state, (0, 1, 2))
    lower = [neighbour(padded_state, dim, 0, (0, 1, 2)) for dim in (0, 1, 2)]
    upper = [neighbour(padded_state, dim, 2, (0, 1, 2)) for dim in (0, 1, 2)]
    slopes = [above - below for above, below in zip(upper, lower)]
    smooth_rate = 0.05
    spread = lower[0] + upper[0] + lower[1] + upper[1] + lower[2] + upper[2] - 6.0 * middle
    return middle - scaled_wind_north * slopes[0] - scaled_wind_east * slopes[1] - scaled_wind_upward * slopes[2] + smooth_rate * spread

def reference(initial_state, scaled_wind_north, scaled_wind_east, scaled_wind_upward):
    for step in range(STEPS):
        initial_state = march_one_step(jnp.pad(initial_state, ((1, 1), (1, 1), (1, 1), (0, 0)), mode='constant'), scaled_wind_north, scaled_wind_east, scaled_wind_upward)
    vertical_mean = lax.optimization_barrier(jnp.mean(initial_state, axis=1, keepdims=True))
    symmetric_slope = initial_state - vertical_mean
    line_variance = lax.optimization_barrier(jnp.mean(symmetric_slope * symmetric_slope, axis=1, keepdims=True))
    normalised_state = symmetric_slope * lax.rsqrt(line_variance + 0.0001)
    return (normalised_state, initial_state)
```

```python
import functools

import jax
import jax.numpy as jnp
from jax import lax
from jax.experimental import pallas as pl
from jax.experimental.pallas import tpu as pltpu
from jax.sharding import PartitionSpec as P

STEPS = 4
CHUNKS = 4
UNROLL = 8
MESH = pl.DeviceIdType.MESH


def march(cur, ahead, behind, east, west, above, below, wind_n, wind_e, wind_u, sign):
    spread = ahead + behind + east + west + above + below
    new = 0.7 * cur + 0.05 * spread
    new = new - (sign * wind_n) * (ahead - behind)
    new = new - wind_e * (east - west)
    return new - wind_u * (above - below)


def advance(
    state, north, east, upward, end, stats,
    field, winds, face, halo, mine, theirs,
    load_sem, slow_s, slow_r, fast_s, fast_r, lon_s, lon_r, lev_s, lev_r, stat_s, stat_r,
):
    planes, length, depth, members = state.shape
    lat, lon, lev = (lax.axis_index(a) for a in ("lat", "lon", "lev"))
    n_lat, n_lon, n_lev = (lax.axis_size(a) for a in ("lat", "lon", "lev"))
    core = lax.rem(lat, 2)
    way = 2 * core - 1
    sign = way.astype(jnp.float32)
    slow, fast = lat + way, lat - way
    last = planes - 1
    part = length // CHUNKS

    def row(q):
        return core * q + (1 - core) * (last - q)

    def slot(t, q):
        if q < 0:
            return 2 * planes + 2 * t + 1
        if q > last:
            return 2 * planes + 2 * t
        return planes * (t % 2) + q

    has_slow = jnp.logical_and(slow >= 0, slow < n_lat)
    has_lon = (lon > 0, lon < n_lon - 1)
    has_lev = (lev > 0, lev < n_lev - 1)

    def load(k, q):
        ref = (state, north, east, upward)[k]
        dst = field.at[slot(0, q), pl.ds(1, length)] if k == 0 else winds.at[k - 1, q]
        return pltpu.make_async_copy(ref.at[row(q)], dst, load_sem.at[k, q])

    order = [last, *range(last)]
    for q in order:
        load(0, q).start()
    for q in [*range(last), last]:
        for k in (1, 2, 3):
            load(k, q).start()

    barrier = pltpu.get_barrier_semaphore()

    def greet(**there):
        pl.semaphore_signal(barrier, inc=1, device_id=there, device_id_type=MESH)

    greet(lat=fast)
    pl.when(has_slow)(lambda: greet(lat=slow))
    for d in range(1, n_lon):
        greet(lon=lax.rem(lon + d, n_lon))
    pl.when(has_lev[0])(lambda: greet(lev=lev - 1))
    pl.when(has_lev[1])(lambda: greet(lev=lev + 1))
    count = n_lon + sum(h.astype(jnp.int32) for h in (has_slow, *has_lev))
    pl.semaphore_wait(barrier, count)

    def to_slow(t, c):
        xs = pl.ds(1 + c * part, part)
        return pltpu.make_async_remote_copy(
            field.at[slot(t, last), xs], field.at[slot(t, planes), xs],
            slow_s.at[t, c], slow_r.at[t, c], device_id={"lat": slow}, device_id_type=MESH,
        )

    def to_fast(t):
        xs = pl.ds(1, length)
        return pltpu.make_async_remote_copy(
            field.at[slot(t, 0), xs], field.at[slot(t, -1), xs],
            fast_s.at[t], fast_r.at[t], device_id={"lat": fast}, device_id_type=MESH,
        )

    groups = (pl.ds(0, last), pl.ds(last, 1))
    slots = lambda t, g: pl.ds(slot(t, 0), last) if g == 0 else pl.ds(slot(t, last), 1)

    def to_lon(t, side, g):
        src, dst = (1, length + 1) if side == 0 else (length, 0)
        return pltpu.make_async_remote_copy(
            field.at[slots(t, g), src], field.at[slots(t, g), dst],
            lon_s.at[t, side, g], lon_r.at[t, side, g],
            device_id={"lon": lon - 1 if side == 0 else lon + 1}, device_id_type=MESH,
        )

    def to_lev(t, side, g):
        return pltpu.make_async_remote_copy(
            face.at[t, side, groups[g]], halo.at[t, 1 - side, groups[g]],
            lev_s.at[t, side, g], lev_r.at[t, side, g],
            device_id={"lev": lev - 1 if side == 0 else lev + 1}, device_id_type=MESH,
        )

    def to_stat(d, g):
        return pltpu.make_async_remote_copy(
            mine.at[groups[g]], theirs.at[n_lon - 1 - d, groups[g]],
            stat_s.at[g, d - 1], stat_r.at[g, n_lon - 1 - d],
            device_id={"lon": lax.rem(lon + d, n_lon)}, device_id_type=MESH,
        )

    def start_edges(t, g):
        for side in (0, 1):
            pl.when(has_lon[side])(lambda: to_lon(t, side, g).start())
            pl.when(has_lev[side])(lambda: to_lev(t, side, g).start())

    def wait_edges(t, g):
        for side in (0, 1):
            pl.when(has_lon[1 - side])(lambda: to_lon(t, side, g).wait_recv())
            pl.when(has_lev[1 - side])(lambda: to_lev(t, side, g).wait_recv())

    def wait_edges_sent(t, g):
        for side in (0, 1):
            pl.when(has_lon[side])(lambda: to_lon(t, side, g).wait_send())
            pl.when(has_lev[side])(lambda: to_lev(t, side, g).wait_send())

    def clear(ref, index, n):
        def body(i, _):
            ref[(*index, i)] = jnp.zeros(ref.shape[len(index) + 1 :], ref.dtype)
            return 0

        lax.fori_loop(0, n, body, 0)

    edge_rows = (0, length + 1)
    for side in (0, 1):

        @pl.when(jnp.logical_not(has_lon[side]))
        def _(side=side):
            for s in range(2 * planes):
                field[s, edge_rows[side]] = jnp.zeros((depth, members), jnp.float32)

        @pl.when(jnp.logical_not(has_lev[side]))
        def _(side=side):
            for t in range(STEPS):
                clear(halo, (t, side), planes)

    load(0, last).wait()
    for c in range(CHUNKS):
        pl.when(has_slow)(lambda: to_slow(0, c).start())
    load(0, 0).wait()
    to_fast(0).start()
    for q in range(1, last):
        load(0, q).wait()

    def pack(t, q):
        def body(i, _):
            for j in range(UNROLL):
                x = i * UNROLL + j
                face[t, 0, q, pl.ds(x, 1), :] = field[slot(t, q), 1 + x, pl.ds(0, 1), :]
                face[t, 1, q, pl.ds(x, 1), :] = field[slot(t, q), 1 + x, pl.ds(depth - 1, 1), :]
            return 0

        lax.fori_loop(0, length // UNROLL, body, 0)

    for q in range(planes):
        pack(0, q)
    for g in (0, 1):
        start_edges(0, g)

    @pl.when(jnp.logical_not(has_slow))
    def _():
        for t in range(STEPS):
            clear(field, (slot(t, planes),), length + 2)

    level = lax.broadcasted_iota(jnp.int32, (depth, members), 0)

    def cells(t, q, x):
        here = slot(t, q)
        cur = field[here, x + 1]
        below = jnp.where(level == 0, halo[t, 0, q, pl.ds(x, 1), :], pltpu.roll(cur, 1, 0))
        above = jnp.where(
            level == depth - 1, halo[t, 1, q, pl.ds(x, 1), :], pltpu.roll(cur, depth - 1, 0)
        )
        return march(
            cur, field[slot(t, q + 1), x + 1], field[slot(t, q - 1), x + 1],
            field[here, x + 2], field[here, x], above, below,
            winds[0, q, x], winds[1, q, x], winds[2, q, x], sign,
        )

    def run(t, q, first, n):
        def body(i, _):
            for j in range(UNROLL):
                x = first + i * UNROLL + j
                new = cells(t, q, x)
                field[slot(t + 1, q), x + 1] = new
                face[t + 1, 0, q, pl.ds(x, 1), :] = new[:1]
                face[t + 1, 1, q, pl.ds(x, 1), :] = new[depth - 1 :]
            return 0

        lax.fori_loop(0, n // UNROLL, body, 0)

    def run_end(t, q, first, n, sums):
        guess = field[slot(t, q), length // 2]

        def body(i, sums):
            total, squares = sums
            for j in range(UNROLL):
                x = first + i * UNROLL + j
                new = cells(t, q, x)
                end[row(q), x] = new
                moved = new - guess
                total = total + moved
                squares = squares + moved * moved
            return total, squares

        return lax.fori_loop(0, n // UNROLL, body, sums)

    def summarise(t, q, sums):
        total, squares = sums
        guess = field[slot(t, q), length // 2]
        mean = total * (1.0 / length)
        mine[q, 0] = guess + mean
        mine[q, 1] = squares - total * mean

    zero = jnp.zeros((depth, members), jnp.float32)
    for t in range(STEPS):
        final = t == STEPS - 1
        if t > 0:
            to_fast(t - 1).wait_send()
        to_fast(t).wait_recv()
        for g in (0, 1):
            wait_edges(t, g)
            if t > 0:
                wait_edges_sent(t - 1, g)
        for q in range(last):
            if t == 0:
                for k in (1, 2, 3):
                    load(k, q).wait()
            if final:
                summarise(t, q, run_end(t, q, 0, length, (zero, zero)))
            else:
                run(t, q, 0, length)
                if q == 0:
                    to_fast(t + 1).start()
        if final:
            for d in range(1, n_lon):
                to_stat(d, 0).start()
        else:
            start_edges(t + 1, 0)
        if t == 0:
            for k in (1, 2, 3):
                load(k, last).wait()
        sums = (zero, zero)
        for c in range(CHUNKS):

            @pl.when(has_slow)
            def _(c=c):
                if t > 0:
                    to_slow(t - 1, c).wait_send()
                to_slow(t, c).wait_recv()

            if final:
                sums = run_end(t, last, c * part, part, sums)
            else:
                run(t, last, c * part, part)
                pl.when(has_slow)(lambda: to_slow(t + 1, c).start())
        if final:
            summarise(t, last, sums)
            for d in range(1, n_lon):
                to_stat(d, 1).start()
        else:
            start_edges(t + 1, 1)

    t = STEPS - 1
    for c in range(CHUNKS):
        pl.when(has_slow)(lambda: to_slow(t, c).wait_send())
    to_fast(t).wait_send()
    for g in (0, 1):
        wait_edges_sent(t, g)
    for g in (0, 1):
        for d in range(1, n_lon):
            to_stat(d, g).wait()
    for q in range(planes):
        means = [mine[q, 0], *(theirs[d, q, 0] for d in range(n_lon - 1))]
        parts = [mine[q, 1], *(theirs[d, q, 1] for d in range(n_lon - 1))]
        mean = sum(means) * (1.0 / n_lon)
        apart = sum((m - mean) * (m - mean) for m in means)
        variance = (sum(parts) + length * apart) * (1.0 / (length * n_lon))
        stats[row(q), 0] = mean
        stats[row(q), 1] = lax.rsqrt(variance + 0.0001)


def normalise(end, stats, normalised, final, scratch, sem):
    planes, length = end.shape[:2]
    copies = [pltpu.make_async_copy(end, final, sem.at[planes])]
    copies[0].start()
    for p in range(planes):
        mean, scale = stats[p, 0], stats[p, 1]

        def body(i, _, p=p, mean=mean, scale=scale):
            for j in range(UNROLL):
                x = i * UNROLL + j
                scratch[p, x] = (end[p, x] - mean) * scale
            return 0

        lax.fori_loop(0, length // UNROLL, body, 0)
        copies.append(pltpu.make_async_copy(scratch.at[p], normalised.at[p], sem.at[p]))
        copies[-1].start()
    for copy in copies:
        copy.wait()


def shards(initial_state, wind_north, wind_east, wind_upward):
    planes, length, depth, members = initial_state.shape
    n_lon = lax.axis_size("lon")
    block = initial_state.shape
    f32 = jnp.float32
    dma = pltpu.SemaphoreType.DMA
    anywhere = pl.BlockSpec(memory_space=pl.ANY)
    vmem = pl.BlockSpec(memory_space=pltpu.VMEM)
    end, stats = pl.pallas_call(
        advance,
        out_shape=(
            pltpu.VMEM(block, f32),
            pltpu.VMEM((planes, 2, depth, members), f32),
        ),
        in_specs=[anywhere] * 4,
        out_specs=(vmem, vmem),
        scratch_shapes=[
            pltpu.VMEM((2 * planes + 2 * STEPS, length + 2, depth, members), f32),
            pltpu.VMEM((3, *block), f32),
            pltpu.VMEM((STEPS, 2, planes, length, members), f32),
            pltpu.VMEM((STEPS, 2, planes, length, members), f32),
            pltpu.VMEM((planes, 2, depth, members), f32),
            pltpu.VMEM((n_lon - 1, planes, 2, depth, members), f32),
            dma((4, planes)),
            dma((STEPS, CHUNKS)), dma((STEPS, CHUNKS)),
            dma((STEPS,)), dma((STEPS,)),
            dma((STEPS, 2, 2)), dma((STEPS, 2, 2)),
            dma((STEPS, 2, 2)), dma((STEPS, 2, 2)),
            dma((2, n_lon - 1)), dma((2, n_lon - 1)),
        ],
        compiler_params=pltpu.CompilerParams(
            collective_id=0, has_side_effects=True, vmem_limit_bytes=54 * 1024 * 1024
        ),
        name="advance",
    )(initial_state, wind_north, wind_east, wind_upward)
    end, stats = (pltpu.with_memory_space_constraint(a, pltpu.VMEM) for a in (end, stats))
    return pl.pallas_call(
        normalise,
        out_shape=(jax.ShapeDtypeStruct(block, f32), jax.ShapeDtypeStruct(block, f32)),
        in_specs=[vmem, vmem],
        out_specs=(anywhere, anywhere),
        scratch_shapes=[pltpu.VMEM(block, f32), dma((planes + 1,))],
        compiler_params=pltpu.CompilerParams(vmem_limit_bytes=32 * 1024 * 1024),
        name="normalise",
    )(end, stats)


def solution(mesh):
    spec = P("lat", "lon", "lev", None)
    return jax.shard_map(
        shards, mesh=mesh, in_specs=(spec,) * 4, out_specs=(spec, spec), check_vma=False
    )
```

```python
import functools

import jax
import jax.numpy as jnp
from jax import lax
from jax.experimental import pallas as pl
from jax.experimental.pallas import tpu as pltpu
from jax.sharding import PartitionSpec as P

STEPS = 4
CHUNKS = 4
UNROLL = 8
UNROLL_PIECE = 24
PARTS = 2
MESH = pl.DeviceIdType.MESH


def march(cur, ahead, behind, east, west, above, below, wind_n, wind_e, wind_u, sign):
    spread = ahead + behind + east + west + above + below
    new = 0.7 * cur + 0.05 * spread
    new = new - (sign * wind_n) * (ahead - behind)
    new = new - wind_e * (east - west)
    return new - wind_u * (above - below)


def advance(
    state, north, east, upward, end, stats,
    field, winds, face, halo, mine, theirs,
    load_sem, piece_sem, slow_s, slow_r, fast_s, fast_r, lon_s, lon_r, lev_s, lev_r, stat_s, stat_r, above_sem,
):
    planes, length, depth, members = state.shape
    lat, lon, lev = (lax.axis_index(a) for a in ("lat", "lon", "lev"))
    n_lat, n_lon, n_lev = (lax.axis_size(a) for a in ("lat", "lon", "lev"))
    core = lax.rem(lat, 2)
    way = 2 * core - 1
    sign = way.astype(jnp.float32)
    slow, fast = lat + way, lat - way
    last = planes - 1
    part = depth // CHUNKS

    def row(q):
        return core * q + (1 - core) * (last - q)

    def slot(t, q):
        if q < 0:
            return 2 * planes + 2 * t + 1
        if q > last:
            return 2 * planes + 2 * t
        return planes * (t % 2) + q

    has_slow = jnp.logical_and(slow >= 0, slow < n_lat)
    has_lon = (lon > 0, lon < n_lon - 1)
    has_lev = (lev > 0, lev < n_lev - 1)

    def load(k, q):
        ref = (state, north, east, upward)[k]
        dst = field.at[slot(0, q), pl.ds(1, length)] if k == 0 else winds.at[k - 1, q]
        return pltpu.make_async_copy(ref.at[row(q)], dst, load_sem.at[k, q])

    def load_piece(c):
        zs = pl.ds(c * part, part)
        return pltpu.make_async_copy(
            state.at[row(last), :, zs],
            field.at[slot(0, last), pl.ds(1, length), zs],
            piece_sem.at[c],
        )

    load_piece(0).start()

    barrier = pltpu.get_barrier_semaphore()

    def greet(**there):
        pl.semaphore_signal(barrier, inc=1, device_id=there, device_id_type=MESH)

    greet(lat=fast)
    pl.when(has_slow)(lambda: greet(lat=slow))
    pl.when(has_lon[1])(lambda: greet(lon=lon + 1))
    pl.when(has_lev[1])(lambda: greet(lev=lev + 1))
    count = 1 + sum(h.astype(jnp.int32) for h in (has_slow, has_lon[0], has_lev[0]))
    load_piece(0).wait()
    for c in range(1, CHUNKS):
        load_piece(c).start()
    pl.semaphore_wait(barrier, count)

    def answer(**there):
        pl.semaphore_signal(above_sem, inc=1, device_id=there, device_id_type=MESH)

    pl.when(has_lon[0])(lambda: answer(lon=lon - 1))
    pl.when(has_lev[0])(lambda: answer(lev=lev - 1))

    def to_slow(t, c):
        xs, zs = pl.ds(1, length), pl.ds(c * part, part)
        return pltpu.make_async_remote_copy(
            field.at[slot(t, last), xs, zs], field.at[slot(t, planes), xs, zs],
            slow_s.at[t, c], slow_r.at[t, c], device_id={"lat": slow}, device_id_type=MESH,
        )

    def to_fast(t):
        xs = pl.ds(1, length)
        return pltpu.make_async_remote_copy(
            field.at[slot(t, 0), xs], field.at[slot(t, -1), xs],
            fast_s.at[t], fast_r.at[t], device_id={"lat": fast}, device_id_type=MESH,
        )

    groups = (pl.ds(0, last), pl.ds(last, 1))
    slots = lambda t, g: pl.ds(slot(t, 0), last) if g == 0 else pl.ds(slot(t, last), 1)

    def to_lon(t, side, g):
        src, dst = (1, length + 1) if side == 0 else (length, 0)
        return pltpu.make_async_remote_copy(
            field.at[slots(t, g), src], field.at[slots(t, g), dst],
            lon_s.at[t, side, g], lon_r.at[t, side, g],
            device_id={"lon": lon - 1 if side == 0 else lon + 1}, device_id_type=MESH,
        )

    def to_lev(t, side, g):
        return pltpu.make_async_remote_copy(
            face.at[t, side, groups[g]], halo.at[t, 1 - side, groups[g]],
            lev_s.at[t, side, g], lev_r.at[t, side, g],
            device_id={"lev": lev - 1 if side == 0 else lev + 1}, device_id_type=MESH,
        )

    def to_stat(d, c):
        where = (slice(0, last),) if c == CHUNKS else (last, slice(None), pl.ds(c * part, part))
        return pltpu.make_async_remote_copy(
            mine.at[where], theirs.at[(n_lon - 1 - d, *where)],
            stat_s.at[c, d - 1], stat_r.at[c, n_lon - 1 - d],
            device_id={"lon": lax.rem(lon + d, n_lon)}, device_id_type=MESH,
        )

    def start_edges(t, g):
        for side in (0, 1):
            pl.when(has_lon[side])(lambda: to_lon(t, side, g).start())
            pl.when(has_lev[side])(lambda: to_lev(t, side, g).start())

    def wait_edges(t, g):
        for side in (0, 1):
            pl.when(has_lon[1 - side])(lambda: to_lon(t, side, g).wait_recv())
            pl.when(has_lev[1 - side])(lambda: to_lev(t, side, g).wait_recv())

    def wait_edges_sent(t, g):
        for side in (0, 1):
            pl.when(has_lon[side])(lambda: to_lon(t, side, g).wait_send())
            pl.when(has_lev[side])(lambda: to_lev(t, side, g).wait_send())

    for c in range(CHUNKS):
        if c > 0:
            load_piece(c).wait()
        pl.when(has_slow)(lambda: to_slow(0, c).start())
    for q in range(last):
        load(0, q).start()
    for q in range(planes):
        for k in (1, 2, 3):
            load(k, q).start()

    def clear(ref, index, n):
        def body(i, _):
            ref[(*index, i)] = jnp.zeros(ref.shape[len(index) + 1 :], ref.dtype)
            return 0

        lax.fori_loop(0, n, body, 0)

    edge_rows = (0, length + 1)
    for side in (0, 1):

        @pl.when(jnp.logical_not(has_lon[side]))
        def _(side=side):
            for s in range(2 * planes):
                field[s, edge_rows[side]] = jnp.zeros((depth, members), jnp.float32)

        @pl.when(jnp.logical_not(has_lev[side]))
        def _(side=side):
            for t in range(STEPS):
                clear(halo, (t, side), planes)

    load(0, 0).wait()
    to_fast(0).start()
    for q in range(1, last):
        load(0, q).wait()

    def pack(t, q):
        def body(i, _):
            for j in range(UNROLL):
                x = i * UNROLL + j
                face[t, 0, q, pl.ds(x, 1), :] = field[slot(t, q), 1 + x, pl.ds(0, 1), :]
                face[t, 1, q, pl.ds(x, 1), :] = field[slot(t, q), 1 + x, pl.ds(depth - 1, 1), :]
            return 0

        lax.fori_loop(0, length // UNROLL, body, 0)

    for q in range(planes):
        pack(0, q)
    answers = has_lon[1].astype(jnp.int32) + has_lev[1].astype(jnp.int32)
    pl.when(answers > 0)(lambda: pl.semaphore_wait(above_sem, answers))
    for g in (0, 1):
        start_edges(0, g)

    @pl.when(jnp.logical_not(has_slow))
    def _():
        for t in range(STEPS):
            clear(field, (slot(t, planes),), length + 2)

    def cells(t, q, x, z, rows):
        here, zs = slot(t, q), pl.ds(z, rows)
        level = lax.broadcasted_iota(jnp.int32, (rows, members), 0)
        cur = field[here, x + 1, zs]
        if z == 0:
            low = halo[t, 0, q, pl.ds(x, 1), :]
        else:
            low = field[here, x + 1, pl.ds(z - 1, 1), :]
        if z + rows == depth:
            high = halo[t, 1, q, pl.ds(x, 1), :]
        else:
            high = field[here, x + 1, pl.ds(z + rows, 1), :]
        below = jnp.where(level == 0, low, pltpu.roll(cur, 1, 0))
        above = jnp.where(level == rows - 1, high, pltpu.roll(cur, rows - 1, 0))
        return march(
            cur, field[slot(t, q + 1), x + 1, zs], field[slot(t, q - 1), x + 1, zs],
            field[here, x + 2, zs], field[here, x, zs], above, below,
            winds[0, q, x, zs], winds[1, q, x, zs], winds[2, q, x, zs], sign,
        )

    def run(t, q, z, rows):
        width = UNROLL if rows == depth else UNROLL_PIECE

        def body(i, _):
            for j in range(width):
                x = i * width + j
                new = cells(t, q, x, z, rows)
                field[slot(t + 1, q), x + 1, pl.ds(z, rows)] = new
                if z == 0:
                    face[t + 1, 0, q, pl.ds(x, 1), :] = new[:1]
                if z + rows == depth:
                    face[t + 1, 1, q, pl.ds(x, 1), :] = new[rows - 1 :]
            return 0

        lax.fori_loop(0, length // width, body, 0)

    def run_end(t, q, z, rows):
        width = UNROLL if rows == depth else UNROLL_PIECE
        zs = pl.ds(z, rows)
        guess = field[slot(t, q), length // 2, zs]

        def body(i, sums):
            total, squares = sums
            for j in range(width):
                x = i * width + j
                new = cells(t, q, x, z, rows)
                end[row(q), x, zs] = new
                moved = new - guess
                total = total + moved
                squares = squares + moved * moved
            return total, squares

        zero = jnp.zeros((rows, members), jnp.float32)
        total, squares = lax.fori_loop(0, length // width, body, (zero, zero))
        mean = total * (1.0 / length)
        mine[q, 0, zs] = guess + mean
        mine[q, 1, zs] = squares - total * mean

    def combine(q, z, rows):
        zs = pl.ds(z, rows)
        means = [mine[q, 0, zs], *(theirs[d, q, 0, zs] for d in range(n_lon - 1))]
        parts = [mine[q, 1, zs], *(theirs[d, q, 1, zs] for d in range(n_lon - 1))]
        mean = sum(means) * (1.0 / n_lon)
        apart = sum((m - mean) * (m - mean) for m in means)
        variance = (sum(parts) + length * apart) * (1.0 / (length * n_lon))
        stats[row(q), 0, zs] = mean
        stats[row(q), 1, zs] = lax.rsqrt(variance + 0.0001)

    for t in range(STEPS):
        final = t == STEPS - 1
        if t > 0:
            to_fast(t - 1).wait_send()
        to_fast(t).wait_recv()
        wait_edges(t, 0)
        if t > 0:
            wait_edges_sent(t - 1, 0)
        for q in range(last):
            if t == 0:
                for k in (1, 2, 3):
                    load(k, q).wait()
            if final:
                run_end(t, q, 0, depth)
            else:
                run(t, q, 0, depth)
                if q == 0:
                    to_fast(t + 1).start()
        if final:
            to_fast(t).wait_send()
            for g in (0, 1):
                wait_edges_sent(t, g)
            for d in range(1, n_lon):
                to_stat(d, CHUNKS).start()
        else:
            start_edges(t + 1, 0)
        wait_edges(t, 1)
        if t > 0:
            wait_edges_sent(t - 1, 1)
        if t == 0:
            for k in (1, 2, 3):
                load(k, last).wait()
        for c in range(CHUNKS):

            @pl.when(has_slow)
            def _(c=c):
                if t > 0:
                    to_slow(t - 1, c).wait_send()
                to_slow(t, c).wait_recv()

            if final:
                run_end(t, last, c * part, part)
                for d in range(1, n_lon):
                    to_stat(d, c).start()
                if c == 0:
                    for d in range(1, n_lon):
                        to_stat(d, CHUNKS).wait()
                    for q in range(last):
                        combine(q, 0, depth)
                else:
                    for d in range(1, n_lon):
                        to_stat(d, c - 1).wait()
                    combine(last, (c - 1) * part, part)
            else:
                run(t, last, c * part, part)
                pl.when(has_slow)(lambda: to_slow(t + 1, c).start())
        if not final:
            start_edges(t + 1, 1)

    for c in range(CHUNKS):
        pl.when(has_slow)(lambda: to_slow(t, c).wait_send())
    for d in range(1, n_lon):
        to_stat(d, CHUNKS - 1).wait()
    combine(last, (CHUNKS - 1) * part, part)


def normalise(end, stats, normalised, final, scratch, sem):
    planes, length = end.shape[:2]
    part = length // PARTS
    copies = [
        pltpu.make_async_copy(end.at[p], final.at[p], sem.at[0, p, 0]) for p in range(planes)
    ]
    for copy in copies:
        copy.start()
    for p in range(planes):
        mean, scale = stats[p, 0], stats[p, 1]
        for c in range(PARTS):

            def body(i, _, p=p, c=c, mean=mean, scale=scale):
                for j in range(UNROLL):
                    x = c * part + i * UNROLL + j
                    scratch[p, x] = (end[p, x] - mean) * scale
                return 0

            lax.fori_loop(0, part // UNROLL, body, 0)
            xs = pl.ds(c * part, part)
            copies.append(
                pltpu.make_async_copy(scratch.at[p, xs], normalised.at[p, xs], sem.at[1, p, c])
            )
            copies[-1].start()
    for copy in copies:
        copy.wait()


def shards(initial_state, wind_north, wind_east, wind_upward):
    planes, length, depth, members = initial_state.shape
    n_lon = lax.axis_size("lon")
    block = initial_state.shape
    f32 = jnp.float32
    dma = pltpu.SemaphoreType.DMA
    anywhere = pl.BlockSpec(memory_space=pl.ANY)
    vmem = pl.BlockSpec(memory_space=pltpu.VMEM)
    end, stats = pl.pallas_call(
        advance,
        out_shape=(
            pltpu.VMEM(block, f32),
            pltpu.VMEM((planes, 2, depth, members), f32),
        ),
        in_specs=[anywhere] * 4,
        out_specs=(vmem, vmem),
        scratch_shapes=[
            pltpu.VMEM((2 * planes + 2 * STEPS, length + 2, depth, members), f32),
            pltpu.VMEM((3, *block), f32),
            pltpu.VMEM((STEPS, 2, planes, length, members), f32),
            pltpu.VMEM((STEPS, 2, planes, length, members), f32),
            pltpu.VMEM((planes, 2, depth, members), f32),
            pltpu.VMEM((n_lon - 1, planes, 2, depth, members), f32),
            dma((4, planes)),
            dma((CHUNKS,)),
            dma((STEPS, CHUNKS)), dma((STEPS, CHUNKS)),
            dma((STEPS,)), dma((STEPS,)),
            dma((STEPS, 2, 2)), dma((STEPS, 2, 2)),
            dma((STEPS, 2, 2)), dma((STEPS, 2, 2)),
            dma((CHUNKS + 1, n_lon - 1)), dma((CHUNKS + 1, n_lon - 1)),
            pltpu.SemaphoreType.REGULAR,
        ],
        compiler_params=pltpu.CompilerParams(
            collective_id=0, has_side_effects=True, vmem_limit_bytes=54 * 1024 * 1024
        ),
        name="advance",
    )(initial_state, wind_north, wind_east, wind_upward)
    end, stats = (pltpu.with_memory_space_constraint(a, pltpu.VMEM) for a in (end, stats))
    return pl.pallas_call(
        normalise,
        out_shape=(jax.ShapeDtypeStruct(block, f32), jax.ShapeDtypeStruct(block, f32)),
        in_specs=[vmem, vmem],
        out_specs=(anywhere, anywhere),
        scratch_shapes=[pltpu.VMEM(block, f32), dma((2, planes, PARTS))],
        compiler_params=pltpu.CompilerParams(vmem_limit_bytes=32 * 1024 * 1024),
        name="normalise",
    )(end, stats)


def solution(mesh):
    spec = P("lat", "lon", "lev", None)
    return jax.shard_map(
        shards, mesh=mesh, in_specs=(spec,) * 4, out_specs=(spec, spec), check_vma=False
    )
```

```python
import functools

import jax
import jax.numpy as jnp
from jax import lax
from jax.experimental import pallas as pl
from jax.experimental.pallas import tpu as pltpu
from jax.sharding import PartitionSpec as P

STEPS = 4
CHUNKS = 4
UNROLL = 8
UNROLL_PIECE = 24
PARTS = 2
MESH = pl.DeviceIdType.MESH


def march(cur, ahead, behind, east, west, above, below, wind_n, wind_e, wind_u, sign):
    spread = ahead + behind + east + west + above + below
    new = 0.7 * cur + 0.05 * spread
    new = new - (sign * wind_n) * (ahead - behind)
    new = new - wind_e * (east - west)
    return new - wind_u * (above - below)


def advance(
    state, north, east, upward, end, stats,
    field, winds, face, halo, mine, theirs,
    load_sem, piece_sem, slow_s, slow_r, fast_s, fast_r, lon_s, lon_r, lev_s, lev_r, stat_s, stat_r, above_sem,
):
    planes, length, depth, members = state.shape
    lat, lon, lev = (lax.axis_index(a) for a in ("lat", "lon", "lev"))
    n_lat, n_lon, n_lev = (lax.axis_size(a) for a in ("lat", "lon", "lev"))
    core = lax.rem(lat, 2)
    way = 2 * core - 1
    sign = way.astype(jnp.float32)
    slow, fast = lat + way, lat - way
    last = planes - 1
    part = depth // CHUNKS

    def row(q):
        return core * q + (1 - core) * (last - q)

    def slot(t, q):
        if q < 0:
            return 2 * planes + 2 * t + 1
        if q > last:
            return 2 * planes + 2 * t
        return planes * (t % 2) + q

    has_slow = jnp.logical_and(slow >= 0, slow < n_lat)
    has_lon = (lon > 0, lon < n_lon - 1)
    has_lev = (lev > 0, lev < n_lev - 1)

    def load(k, q):
        ref = (state, north, east, upward)[k]
        dst = field.at[slot(0, q), pl.ds(1, length)] if k == 0 else winds.at[k - 1, q]
        return pltpu.make_async_copy(ref.at[row(q)], dst, load_sem.at[k, q])

    def load_piece(c):
        zs = pl.ds(c * part, part)
        return pltpu.make_async_copy(
            state.at[row(last), :, zs],
            field.at[slot(0, last), pl.ds(1, length), zs],
            piece_sem.at[c],
        )

    load_piece(0).start()

    barrier = pltpu.get_barrier_semaphore()

    def greet(**there):
        pl.semaphore_signal(barrier, inc=1, device_id=there, device_id_type=MESH)

    greet(lat=fast)
    pl.when(has_slow)(lambda: greet(lat=slow))
    pl.when(has_lon[1])(lambda: greet(lon=lon + 1))
    pl.when(has_lev[1])(lambda: greet(lev=lev + 1))
    count = 1 + sum(h.astype(jnp.int32) for h in (has_slow, has_lon[0], has_lev[0]))
    load_piece(0).wait()
    for c in range(1, CHUNKS):
        load_piece(c).start()
    pl.semaphore_wait(barrier, count)

    def answer(**there):
        pl.semaphore_signal(above_sem, inc=1, device_id=there, device_id_type=MESH)

    pl.when(has_lon[0])(lambda: answer(lon=lon - 1))
    pl.when(has_lev[0])(lambda: answer(lev=lev - 1))

    def pieces(t, c):
        if t == STEPS - 1 and c == CHUNKS - 1:
            return ((c, 0, length // 2), (CHUNKS, length // 2, length // 2))
        return ((c, 0, length),)

    def to_slow(t, c, piece):
        s, x, n = piece
        xs, zs = pl.ds(1 + x, n), pl.ds(c * part, part)
        return pltpu.make_async_remote_copy(
            field.at[slot(t, last), xs, zs], field.at[slot(t, planes), xs, zs],
            slow_s.at[t, s], slow_r.at[t, s], device_id={"lat": slow}, device_id_type=MESH,
        )

    def to_fast(t):
        xs = pl.ds(1, length)
        return pltpu.make_async_remote_copy(
            field.at[slot(t, 0), xs], field.at[slot(t, -1), xs],
            fast_s.at[t], fast_r.at[t], device_id={"lat": fast}, device_id_type=MESH,
        )

    groups = (pl.ds(0, last), pl.ds(last, 1))
    slots = lambda t, g: pl.ds(slot(t, 0), last) if g == 0 else pl.ds(slot(t, last), 1)

    def to_lon(t, side, g):
        src, dst = (1, length + 1) if side == 0 else (length, 0)
        return pltpu.make_async_remote_copy(
            field.at[slots(t, g), src], field.at[slots(t, g), dst],
            lon_s.at[t, side, g], lon_r.at[t, side, g],
            device_id={"lon": lon - 1 if side == 0 else lon + 1}, device_id_type=MESH,
        )

    def to_lev(t, side, g):
        return pltpu.make_async_remote_copy(
            face.at[t, side, groups[g]], halo.at[t, 1 - side, groups[g]],
            lev_s.at[t, side, g], lev_r.at[t, side, g],
            device_id={"lev": lev - 1 if side == 0 else lev + 1}, device_id_type=MESH,
        )

    def to_stat(d, c):
        where = (slice(0, last),) if c == CHUNKS else (last, slice(None), pl.ds(c * part, part))
        return pltpu.make_async_remote_copy(
            mine.at[where], theirs.at[(n_lon - 1 - d, *where)],
            stat_s.at[c, d - 1], stat_r.at[c, n_lon - 1 - d],
            device_id={"lon": lax.rem(lon + d, n_lon)}, device_id_type=MESH,
        )

    def start_edges(t, g):
        for side in (0, 1):
            pl.when(has_lon[side])(lambda: to_lon(t, side, g).start())
            pl.when(has_lev[side])(lambda: to_lev(t, side, g).start())

    def wait_edges(t, g):
        for side in (0, 1):
            pl.when(has_lon[1 - side])(lambda: to_lon(t, side, g).wait_recv())
            pl.when(has_lev[1 - side])(lambda: to_lev(t, side, g).wait_recv())

    def wait_edges_sent(t, g):
        for side in (0, 1):
            pl.when(has_lon[side])(lambda: to_lon(t, side, g).wait_send())
            pl.when(has_lev[side])(lambda: to_lev(t, side, g).wait_send())

    for c in range(CHUNKS):
        if c > 0:
            load_piece(c).wait()
        pl.when(has_slow)(lambda: to_slow(0, c, *pieces(0, c)).start())
    for q in range(last):
        load(0, q).start()
    for q in range(planes):
        for k in (1, 2, 3):
            load(k, q).start()

    def clear(ref, index, n):
        def body(i, _):
            ref[(*index, i)] = jnp.zeros(ref.shape[len(index) + 1 :], ref.dtype)
            return 0

        lax.fori_loop(0, n, body, 0)

    edge_rows = (0, length + 1)
    for side in (0, 1):

        @pl.when(jnp.logical_not(has_lon[side]))
        def _(side=side):
            for s in range(2 * planes):
                field[s, edge_rows[side]] = jnp.zeros((depth, members), jnp.float32)

        @pl.when(jnp.logical_not(has_lev[side]))
        def _(side=side):
            for t in range(STEPS):
                clear(halo, (t, side), planes)

    load(0, 0).wait()
    to_fast(0).start()
    for q in range(1, last):
        load(0, q).wait()

    def pack(t, q):
        def body(i, _):
            for j in range(UNROLL):
                x = i * UNROLL + j
                face[t, 0, q, pl.ds(x, 1), :] = field[slot(t, q), 1 + x, pl.ds(0, 1), :]
                face[t, 1, q, pl.ds(x, 1), :] = field[slot(t, q), 1 + x, pl.ds(depth - 1, 1), :]
            return 0

        lax.fori_loop(0, length // UNROLL, body, 0)

    for q in range(planes):
        pack(0, q)
    answers = has_lon[1].astype(jnp.int32) + has_lev[1].astype(jnp.int32)
    pl.when(answers > 0)(lambda: pl.semaphore_wait(above_sem, answers))
    for g in (0, 1):
        start_edges(0, g)

    @pl.when(jnp.logical_not(has_slow))
    def _():
        for t in range(STEPS):
            clear(field, (slot(t, planes),), length + 2)

    def cells(t, q, x, z, rows):
        here, zs = slot(t, q), pl.ds(z, rows)
        level = lax.broadcasted_iota(jnp.int32, (rows, members), 0)
        cur = field[here, x + 1, zs]
        if z == 0:
            low = halo[t, 0, q, pl.ds(x, 1), :]
        else:
            low = field[here, x + 1, pl.ds(z - 1, 1), :]
        if z + rows == depth:
            high = halo[t, 1, q, pl.ds(x, 1), :]
        else:
            high = field[here, x + 1, pl.ds(z + rows, 1), :]
        below = jnp.where(level == 0, low, pltpu.roll(cur, 1, 0))
        above = jnp.where(level == rows - 1, high, pltpu.roll(cur, rows - 1, 0))
        return march(
            cur, field[slot(t, q + 1), x + 1, zs], field[slot(t, q - 1), x + 1, zs],
            field[here, x + 2, zs], field[here, x, zs], above, below,
            winds[0, q, x, zs], winds[1, q, x, zs], winds[2, q, x, zs], sign,
        )

    def run(t, q, z, rows):
        width = UNROLL if rows == depth else UNROLL_PIECE

        def body(i, _):
            for j in range(width):
                x = i * width + j
                new = cells(t, q, x, z, rows)
                field[slot(t + 1, q), x + 1, pl.ds(z, rows)] = new
                if z == 0:
                    face[t + 1, 0, q, pl.ds(x, 1), :] = new[:1]
                if z + rows == depth:
                    face[t + 1, 1, q, pl.ds(x, 1), :] = new[rows - 1 :]
            return 0

        lax.fori_loop(0, length // width, body, 0)

    def run_end(t, q, z, rows, first, n, sums):
        width = UNROLL if rows == depth else UNROLL_PIECE
        zs = pl.ds(z, rows)
        guess = field[slot(t, q), length // 2, zs]

        def body(i, sums):
            total, squares = sums
            for j in range(width):
                x = first + i * width + j
                new = cells(t, q, x, z, rows)
                end[row(q), x, zs] = new
                moved = new - guess
                total = total + moved
                squares = squares + moved * moved
            return total, squares

        if sums is None:
            sums = (jnp.zeros((rows, members), jnp.float32),) * 2
        total, squares = sums = lax.fori_loop(0, n // width, body, sums)
        if first + n < length:
            return sums
        mean = total * (1.0 / length)
        mine[q, 0, zs] = guess + mean
        mine[q, 1, zs] = squares - total * mean

    def combine(q, z, rows):
        zs = pl.ds(z, rows)
        means = [mine[q, 0, zs], *(theirs[d, q, 0, zs] for d in range(n_lon - 1))]
        parts = [mine[q, 1, zs], *(theirs[d, q, 1, zs] for d in range(n_lon - 1))]
        mean = sum(means) * (1.0 / n_lon)
        apart = sum((m - mean) * (m - mean) for m in means)
        variance = (sum(parts) + length * apart) * (1.0 / (length * n_lon))
        stats[row(q), 0, zs] = mean
        stats[row(q), 1, zs] = lax.rsqrt(variance + 0.0001)

    for t in range(STEPS):
        final = t == STEPS - 1
        if t > 0:
            to_fast(t - 1).wait_send()
        to_fast(t).wait_recv()
        wait_edges(t, 0)
        if t > 0:
            wait_edges_sent(t - 1, 0)
        for q in range(last):
            if t == 0:
                for k in (1, 2, 3):
                    load(k, q).wait()
            if final:
                run_end(t, q, 0, depth, 0, length, None)
            else:
                run(t, q, 0, depth)
                if q == 0:
                    to_fast(t + 1).start()
        if final:
            to_fast(t).wait_send()
            for g in (0, 1):
                wait_edges_sent(t, g)
            for d in range(1, n_lon):
                to_stat(d, CHUNKS).start()
        else:
            start_edges(t + 1, 0)
        wait_edges(t, 1)
        if t > 0:
            wait_edges_sent(t - 1, 1)
        if t == 0:
            for k in (1, 2, 3):
                load(k, last).wait()
        for c in range(CHUNKS):

            @pl.when(has_slow)
            def _(c=c):
                if t > 0:
                    to_slow(t - 1, c, *pieces(t - 1, c)).wait_send()
                to_slow(t, c, pieces(t, c)[0]).wait_recv()

            if final:
                sums = None
                for piece in pieces(t, c):
                    if piece[1] > 0:
                        pl.when(has_slow)(lambda: to_slow(t, c, piece).wait_recv())
                    sums = run_end(t, last, c * part, part, *piece[1:], sums)
                for d in sorted(range(1, n_lon), key=lambda d: -min(d, n_lon - d)):
                    to_stat(d, c).start()
                if c == 0:
                    for d in range(1, n_lon):
                        to_stat(d, CHUNKS).wait()
                    for q in range(last):
                        combine(q, 0, depth)
                else:
                    for d in range(1, n_lon):
                        to_stat(d, c - 1).wait()
                    combine(last, (c - 1) * part, part)
            else:
                run(t, last, c * part, part)

                @pl.when(has_slow)
                def _(c=c):
                    for piece in pieces(t + 1, c):
                        to_slow(t + 1, c, piece).start()
        if not final:
            start_edges(t + 1, 1)

    for c in range(CHUNKS):
        for piece in pieces(t, c):
            pl.when(has_slow)(lambda: to_slow(t, c, piece).wait_send())
    for d in range(1, n_lon):
        to_stat(d, CHUNKS - 1).wait()
    combine(last, (CHUNKS - 1) * part, part)


def normalise(end, stats, normalised, final, scratch, sem):
    planes, length = end.shape[:2]
    part = length // PARTS
    copies = [
        pltpu.make_async_copy(end.at[p], final.at[p], sem.at[0, p, 0]) for p in range(planes)
    ]
    for copy in copies:
        copy.start()
    for p in range(planes):
        mean, scale = stats[p, 0], stats[p, 1]
        for c in range(PARTS):

            def body(i, _, p=p, c=c, mean=mean, scale=scale):
                for j in range(UNROLL):
                    x = c * part + i * UNROLL + j
                    scratch[p, x] = (end[p, x] - mean) * scale
                return 0

            lax.fori_loop(0, part // UNROLL, body, 0)
            xs = pl.ds(c * part, part)
            copies.append(
                pltpu.make_async_copy(scratch.at[p, xs], normalised.at[p, xs], sem.at[1, p, c])
            )
            copies[-1].start()
    for copy in copies:
        copy.wait()


def shards(initial_state, wind_north, wind_east, wind_upward):
    planes, length, depth, members = initial_state.shape
    n_lon = lax.axis_size("lon")
    block = initial_state.shape
    f32 = jnp.float32
    dma = pltpu.SemaphoreType.DMA
    anywhere = pl.BlockSpec(memory_space=pl.ANY)
    vmem = pl.BlockSpec(memory_space=pltpu.VMEM)
    end, stats = pl.pallas_call(
        advance,
        out_shape=(
            pltpu.VMEM(block, f32),
            pltpu.VMEM((planes, 2, depth, members), f32),
        ),
        in_specs=[anywhere] * 4,
        out_specs=(vmem, vmem),
        scratch_shapes=[
            pltpu.VMEM((2 * planes + 2 * STEPS, length + 2, depth, members), f32),
            pltpu.VMEM((3, *block), f32),
            pltpu.VMEM((STEPS, 2, planes, length, members), f32),
            pltpu.VMEM((STEPS, 2, planes, length, members), f32),
            pltpu.VMEM((planes, 2, depth, members), f32),
            pltpu.VMEM((n_lon - 1, planes, 2, depth, members), f32),
            dma((4, planes)),
            dma((CHUNKS,)),
            dma((STEPS, CHUNKS + 1)), dma((STEPS, CHUNKS + 1)),
            dma((STEPS,)), dma((STEPS,)),
            dma((STEPS, 2, 2)), dma((STEPS, 2, 2)),
            dma((STEPS, 2, 2)), dma((STEPS, 2, 2)),
            dma((CHUNKS + 1, n_lon - 1)), dma((CHUNKS + 1, n_lon - 1)),
            pltpu.SemaphoreType.REGULAR,
        ],
        compiler_params=pltpu.CompilerParams(
            collective_id=0, has_side_effects=True, vmem_limit_bytes=54 * 1024 * 1024
        ),
        name="advance",
    )(initial_state, wind_north, wind_east, wind_upward)
    end, stats = (pltpu.with_memory_space_constraint(a, pltpu.VMEM) for a in (end, stats))
    return pl.pallas_call(
        normalise,
        out_shape=(jax.ShapeDtypeStruct(block, f32), jax.ShapeDtypeStruct(block, f32)),
        in_specs=[vmem, vmem],
        out_specs=(anywhere, anywhere),
        scratch_shapes=[pltpu.VMEM(block, f32), dma((2, planes, PARTS))],
        compiler_params=pltpu.CompilerParams(vmem_limit_bytes=32 * 1024 * 1024),
        name="normalise",
    )(end, stats)


def solution(mesh):
    spec = P("lat", "lon", "lev", None)
    return jax.shard_map(
        shards, mesh=mesh, in_specs=(spec,) * 4, out_specs=(spec, spec), check_vma=False
    )
```
